32 devices in a mesh: gx: 4 (over y, x), gy: 4 (over z), gz: 2 (over core).
Axes of the slice: x: 2, y: 2, z: 4, core: 2. Of those that a mesh axis runs over, the one named last changes fastest.
Arguments:
- surface_ids: int32 [256, 256, 256], P('gx', 'gy', 'gz'), may hold values from 0 to 256, as said below
- class_map: int32 [256, 256, 256], P('gx', 'gy', 'gz'), may hold values from 0 to 3
- conductivity: float32 [256, 256, 256], P('gx', 'gy', 'gz'), may hold values from 0.5 to 2
- normals: float32 [3, 256], replicated, may hold values from -9 to 9
- class_table: float32 [4], replicated, may hold values from 0.25 to 1
Outputs:
- distance: float32 [256, 256, 256], P('gx', 'gy', 'gz')
The draws below stay inside these ranges and needn't reach their ends.
Inputs may be any that keep to these rules, and one draw needn't show every extreme that they name: `surface_ids`: 0 marks a cell without a source and k a cell of patch k; each cell holds a source with probability one quarter, of a patch drawn evenly.
All inputs are finite; a program needn't handle non-finite values.
Results may differ from the reference program's by a relative error of at most 0.0003.
Values sent between devices are 32-bit elements; how exact they have to be, the bound alone decides.
No kernel may reach another device: no remote copies, remote signals or barrier semaphores. Data moves between devices by JAX's collectives and lax.ppermute only.
A program may use at most 128 MiB of HBM per device.

```python
import math
import jax
import jax.numpy as jnp
from jax import lax

N = 256
STEPS = 8
K = 256
CLASSES = 4


def draw_surface_ids(key, part):
    first_key, second_key = jax.random.split(jax.random.fold_in(key, 11))
    patch_ids = jax.random.randint(first_key, (N, N, N), 1, K + 1)
    keeping = jax.random.randint(second_key, (N, N, N), 0, 4) == 0
    return jnp.where(keeping, patch_ids, 0).astype(jnp.int32)


def touch_ends(array, rng, smallest, largest):
    dims = array.shape
    index_at = [jax.random.randint(jax.random.fold_in(rng, axis), (), 0, dims[axis]) for axis in range(len(dims))]
    array = array.at[tuple(index_at)].set(smallest)
    longest = dims.index(max(dims))
    index_at[longest] = (index_at[longest] + 1) % dims[longest]
    return array.at[tuple(index_at)].set(largest)


def levels(stream_key, shape, cuts, low, largest):
    gain, own = 1.0, jax.random.fold_in(stream_key, 6)
    for position, blocks in cuts:
        steps = jnp.exp(jax.random.uniform(jax.random.fold_in(own, position), (blocks,), jnp.float32, low / len(cuts), largest / len(cuts)))
        gain = gain * jnp.repeat(steps, shape[position] // blocks).reshape([-1 if axis == position else 1 for axis in range(len(shape))])
    return gain


def gaussian(key, shape, spread, limit, kind=jnp.bfloat16):
    return jnp.clip(spread * jax.random.normal(key, shape, jnp.float32), -limit, limit).astype(kind)


def setup_inputs(seed: int = 0) -> dict:
    splits = jax.random.split(jax.random.key(seed), 6)
    surface_ids = draw_surface_ids(jax.random.fold_in(splits[5], 71), 0)
    class_map = touch_ends(jax.random.randint(splits[1], (N, N, N), 0, CLASSES), jax.random.fold_in(splits[1], 1), 0, CLASSES - 1).astype(jnp.int32)
    conductivity = jnp.clip(jnp.exp(math.log(2.0) - 1.3862944 * jax.random.uniform(splits[2], (N, N, N), jnp.float32) ** levels(splits[2], (N, N, N), ((0, 4), (1, 4), (2, 2)), -0.2, 0.2)), 0.5, 2.0)
    normals = gaussian(splits[3], (3, K), 1.5, 9.0, jnp.float32)
    class_table = jnp.clip(jnp.exp(jax.random.uniform(splits[4], (CLASSES,), jnp.float32, math.log(0.25), math.log(1.0))), 0.25, 1.0)
    return {"surface_ids": surface_ids, "class_map": class_map, "conductivity": conductivity, "normals": normals, "class_table": class_table}


time_step = 0.08
norm_floor = 0.5
offsets = ((1, 0, 0), (-1, 0, 0), (0, 1, 0), (0, -1, 0), (0, 0, 1), (0, 0, -1))

def shifted(padded, offset):
    extent = padded.shape[-3:]
    return padded[..., 1 + offset[0]:extent[0] - 1 + offset[0], 1 + offset[1]:extent[1] - 1 + offset[1], 1 + offset[2]:extent[2] - 1 + offset[2]]

def diffuse(padded, root_field):
    center = shifted(padded, (0, 0, 0))
    middle = shifted(root_field, (0, 0, 0))
    inflow = jnp.zeros_like(center)
    for offset in offsets:
        inflow = inflow + shifted(root_field, offset) * (shifted(padded, offset) - center)
    return center + time_step * middle * inflow

def cosine_table(length):
    wave_number = jnp.arange(length, dtype=jnp.float32)[:, None]
    sample = jnp.arange(length, dtype=jnp.float32)[None, :]
    factor = jnp.where(wave_number == 0, jnp.sqrt(1.0 / length), jnp.sqrt(2.0 / length))
    return factor * jnp.cos(jnp.pi * wave_number * (2.0 * sample + 1.0) / (2.0 * length))

def eigen_values(length):
    wave_number = jnp.arange(length, dtype=jnp.float32)
    return 2.0 - 2.0 * jnp.cos(jnp.pi * wave_number / length)

def normalize(heat_field):
    magnitude = jnp.sqrt(heat_field[0] * heat_field[0] + heat_field[1] * heat_field[1] + heat_field[2] * heat_field[2])
    return heat_field / jnp.maximum(magnitude, norm_floor)

def reference(surface_ids, class_map, conductivity, normals, class_table):
    lookup_table = jnp.concatenate([jnp.zeros((3, 1), jnp.float32), normals], axis=1)
    source = jnp.take(lookup_table, surface_ids, axis=1)
    conduct = class_table[class_map] * conductivity
    padded_root = jnp.pad(jnp.sqrt(conduct), 1)

    def evolve(component):
        for step_index in range(STEPS):
            component = diffuse(jnp.pad(component, 1), padded_root)
        return component
    heat_field = lax.map(evolve, source)
    unit_field = normalize(heat_field)
    faces_x = jnp.pad(unit_field[0], ((1, 1), (0, 0), (0, 0)))
    faces_y = jnp.pad(unit_field[1], ((0, 0), (1, 1), (0, 0)))
    faces_z = jnp.pad(unit_field[2], ((0, 0), (0, 0), (1, 1)))
    part_x = 0.5 * (faces_x[2:] - faces_x[:-2])
    part_y = 0.5 * (faces_y[:, 2:] - faces_y[:, :-2])
    part_z = 0.5 * (faces_z[:, :, 2:] - faces_z[:, :, :-2])
    divergence = part_x + part_y + part_z
    cosine = cosine_table(N)
    highest = lax.Precision.HIGHEST
    spectrum = jnp.einsum('kn,nyz->kyz', cosine, divergence, precision=highest)
    spectrum = jnp.einsum('kn,xnz->xkz', cosine, spectrum, precision=highest)
    spectrum = jnp.einsum('kn,xyn->xyk', cosine, spectrum, precision=highest)
    spectra = eigen_values(N)
    screen = 4.0 / (N * N)
    divisor = spectra[:, None, None] + spectra[None, :, None] + spectra[None, None, :] + screen
    solved = -spectrum / divisor
    solved = jnp.einsum('kn,kyz->nyz', cosine, solved, precision=highest)
    solved = jnp.einsum('kn,xkz->xnz', cosine, solved, precision=highest)
    distance = jnp.einsum('kn,xyk->xyn', cosine, solved, precision=highest)
    return distance
```

```python
import functools

import jax
import jax.numpy as jnp
import numpy as np
from jax import lax
from jax.experimental import pallas as pl
from jax.experimental.pallas import tpu as pltpu
from jax.sharding import PartitionSpec as P

STEPS = 8
TIME_STEP = 0.08
NORM_FLOOR = 0.5
LANES = 128
SUBLANES = 8
HALO = STEPS + 1
PAD = 2 * SUBLANES
HIGHEST = lax.Precision.HIGHEST


def cosine_table(length):
    f32 = np.float32
    wave = np.arange(length, dtype=f32)[:, None]
    sample = np.arange(length, dtype=f32)[None, :]
    factor = np.where(wave == 0, np.sqrt(f32(1.0 / length)), np.sqrt(f32(2.0 / length)))
    angle = f32(np.pi) * wave * (f32(2.0) * sample + f32(1.0)) / f32(2.0 * length)
    return (factor * np.cos(angle)).astype(f32)


def eigen_values(length):
    wave = np.arange(length, dtype=np.float32)
    return (np.float32(2.0) - np.float32(2.0) * np.cos(np.float32(np.pi) * wave / np.float32(length))).astype(
        np.float32
    )


def exact_table(length):
    wave = np.arange(length, dtype=np.float64)[:, None]
    sample = np.arange(length, dtype=np.float64)[None, :]
    factor = np.where(wave == 0, np.sqrt(1.0 / length), np.sqrt(2.0 / length))
    return factor * np.cos(np.pi * wave * (2.0 * sample + 1.0) / (2.0 * length))


def dot(a, b):
    return jnp.dot(a, b, precision=HIGHEST, preferred_element_type=jnp.float32)


def dot_nt(a, b):
    return lax.dot_general(
        a, b, (((1,), (1,)), ((), ())), precision=HIGHEST, preferred_element_type=jnp.float32
    )


def halves(values):
    high = values.astype(jnp.bfloat16)
    return high, (values - high.astype(jnp.float32)).astype(jnp.bfloat16)


def table_halves(table):
    table = np.asarray(table, np.float32)
    high = table.astype(jnp.bfloat16)
    return jnp.asarray(np.stack([high, (table - high.astype(np.float32)).astype(jnp.bfloat16)]))


def product(a, b, contract):
    def part(x, y):
        return lax.dot_general(x, y, (contract, ((), ())), preferred_element_type=jnp.float32)

    return part(a[0], b[0]) + (part(a[0], b[1]) + part(a[1], b[0]))


NN = ((1,), (0,))
NT = ((1,), (1,))


def z_neighbours(tiles, first, last):
    below = [pltpu.roll(t, 1, 1) for t in tiles]
    above = [pltpu.roll(t, LANES - 1, 1) for t in tiles]
    count = len(tiles)
    down = [jnp.where(first, below[h - 1] if h else 0.0, below[h]) for h in range(count)]
    up = [jnp.where(last, above[h + 1] if h + 1 < count else 0.0, above[h]) for h in range(count)]
    return up, down


def diffuse_kernel(
    own_ref, west_ref, east_ref, south_ref, north_ref, sw_ref, se_ref, nw_ref, ne_ref, table_ref, cosine_ref,
    out_ref, field_ref, va, vb, keep_ref, gain_ref, za, zb, sems, *, dims
):
    tiles, planes, rows, own_x, own_y, pack, groups = dims
    span = own_y + 2 * SUBLANES
    chunk = pl.ds(SUBLANES, span)
    lane = lax.broadcasted_iota(jnp.int32, (span, LANES), 1)
    first, last = lane == 0, lane == LANES - 1
    table_blocks = table_ref.shape[1]
    every = range(tiles)
    own_rows = pl.ds(PAD, own_y)

    copies = [
        pltpu.make_async_copy(
            ref, field_ref.at[:, :, pl.ds(start, size), own_rows, :], sems.at[n]
        )
        for n, (ref, start, size) in enumerate(
            ((west_ref, 0, HALO), (own_ref, HALO, own_x), (east_ref, HALO + own_x, HALO))
        )
    ]
    for copy in copies:
        copy.start()

    def rim(ref, begin, above):
        def one(x, carry):
            for h in every:
                for f in range(2):
                    if above:
                        eight, single, at = x * HALO, x * HALO + SUBLANES, PAD + own_y
                        far = at + SUBLANES
                    else:
                        eight, single, at = x * HALO + 1, x * HALO, SUBLANES
                        far = at - 1
                    field_ref[h, f, begin + x, pl.ds(at, SUBLANES), :] = ref[
                        h, f, pl.ds(eight, SUBLANES), :
                    ]
                    field_ref[h, f, begin + x, pl.ds(far, 1), :] = ref[h, f, pl.ds(single, 1), :]
            return carry

        lax.fori_loop(0, ref.shape[2] // HALO, one, 0)

    rim(sw_ref, 0, False)
    rim(south_ref, HALO, False)
    rim(se_ref, HALO + own_x, False)
    rim(nw_ref, 0, True)
    rim(north_ref, HALO, True)
    rim(ne_ref, HALO + own_x, True)
    for copy in copies:
        copy.wait()

    row = lax.broadcasted_iota(jnp.int32, (SUBLANES, LANES), 0)

    def spread(x):
        for y in range(rows // SUBLANES):
            at = pl.ds(y * SUBLANES, SUBLANES)
            for h in every:
                ids = field_ref[h, 0, x, at, :]
                root = field_ref[h, 1, x, at, :]
                if y == 0 or y == rows // SUBLANES - 1:
                    inside = row == (SUBLANES - 1 if y == 0 else 0)
                    ids = jnp.where(inside, ids, 0.0)
                    root = jnp.where(inside, root, 0.0)
                ids = ids.astype(jnp.int32)
                low = (ids - 1) & (LANES - 1)
                high = (ids - 1) >> (LANES.bit_length() - 1)
                for c in range(3):
                    value = jnp.zeros((SUBLANES, LANES), jnp.float32)
                    for k in range(table_blocks):
                        found = jnp.take_along_axis(table_ref[c, k], low, axis=1)
                        value = jnp.where(high == k, found, value)
                    va[c, h, x, at, :] = value * root

    def coefficients(x):
        one = jnp.minimum(x, 1)
        mid = [field_ref[h, 1, x, chunk, :] for h in every]
        up, down = z_neighbours(mid, first, last)
        for h in every:
            total = (
                (field_ref[h, 1, x + 1, chunk, :] + field_ref[h, 1, x - 1, chunk, :])
                + (
                    field_ref[h, 1, x, pl.ds(SUBLANES + one, span), :]
                    + field_ref[h, 1, x, pl.ds(SUBLANES - one, span), :]
                )
                + (up[h] + down[h])
            )
            scaled = TIME_STEP * mid[h]
            keep_ref[h, x, chunk, :] = 1.0 - scaled * total
            gain_ref[h, x, chunk, :] = scaled * mid[h]

    def prepare(x, carry):
        spread(x)
        coefficients(x)
        return carry

    spread(0)
    lax.fori_loop(1, planes - 1, prepare, 0)
    spread(planes - 1)

    tile_lane = lax.broadcasted_iota(jnp.int32, (SUBLANES, LANES), 1)
    tile_first, tile_last = tile_lane == 0, tile_lane == LANES - 1

    def along_z(source, x, y, kept):
        at = pl.ds(SUBLANES * (y + 1), SUBLANES)
        for c in range(3):
            up, down = z_neighbours([source[c, h, x, at, :] for h in every], tile_first, tile_last)
            for h in every:
                kept[c, h, pl.ds(y * SUBLANES, SUBLANES), :] = up[h] + down[h]

    def update(source, target, x, y, kept, one):
        base = SUBLANES * (y + 1)
        at = pl.ds(base, SUBLANES)
        for h in every:
            keep, gain = keep_ref[h, x, at, :], gain_ref[h, x, at, :]
            for c in range(3):
                total = (
                    (source[c, h, x + 1, at, :] + source[c, h, x - 1, at, :])
                    + (
                        source[c, h, x, pl.ds(base + one, SUBLANES), :]
                        + source[c, h, x, pl.ds(base - one, SUBLANES), :]
                    )
                    + kept[c, h, pl.ds(y * SUBLANES, SUBLANES), :]
                )
                target[c, h, x, at, :] = keep * source[c, h, x, at, :] + gain * total

    def sweep(source, target, begin):
        for y in range(span // SUBLANES):
            along_z(source, begin, y, za)

        def two_planes(pair, carry):
            x = begin + 2 * pair
            one = jnp.minimum(x, 1)
            for y in range(span // SUBLANES):
                update(source, target, x, y, za, one)
                along_z(source, x + 1, y, zb)
            for y in range(span // SUBLANES):
                update(source, target, x + 1, y, zb, one)
                along_z(source, x + 2, y, za)
            return carry

        lax.fori_loop(0, planes // 2 - begin, two_planes, 0)

    def two_steps(pair, carry):
        sweep(va, vb, 2 * pair + 1)
        sweep(vb, va, 2 * pair + 2)
        return carry

    lax.fori_loop(0, STEPS // 2, two_steps, 0)

    def unit(x, carry):
        for h in every:
            root = field_ref[h, 1, x, chunk, :]
            inverse = jnp.where(root > 0.0, 1.0 / jnp.where(root > 0.0, root, 1.0), 0.0)
            heat = [va[c, h, x, chunk, :] * inverse for c in range(3)]
            size = jnp.sqrt(heat[0] * heat[0] + heat[1] * heat[1] + heat[2] * heat[2])
            scale = 0.5 / jnp.maximum(size, NORM_FLOOR)
            for c in range(3):
                vb[c, h, x, chunk, :] = heat[c] * scale
        return carry

    lax.fori_loop(STEPS, planes - STEPS, unit, 0)

    own_lane = lax.broadcasted_iota(jnp.int32, (own_y, LANES), 1)
    own_first, own_last = own_lane == 0, own_lane == LANES - 1
    block = out_ref.shape[2]
    batch = 2

    def transform(step, carry):
        one = jnp.minimum(step + 1, 1)
        slabs = []
        for j in range(batch * pack):
            x = HALO + step * (batch * pack) + j
            up, down = z_neighbours([vb[2, h, x, own_rows, :] for h in every], own_first, own_last)
            slabs.append(
                jnp.concatenate(
                    [
                        (vb[0, h, x + 1, own_rows, :] - vb[0, h, x - 1, own_rows, :])
                        + (
                            vb[1, h, x, pl.ds(PAD + one, own_y), :]
                            - vb[1, h, x, pl.ds(PAD - one, own_y), :]
                        )
                        + (up[h] - down[h])
                        for h in every
                    ],
                    axis=1,
                )
            )
        lines = halves(jnp.concatenate(slabs, axis=0))
        spectrum = product((cosine_ref[0], cosine_ref[1]), lines, NT)
        for q in range(batch):
            for g in range(groups):
                out_ref[g, step * batch + q] = spectrum[
                    g * block : (g + 1) * block, q * LANES : (q + 1) * LANES
                ]
        return carry

    lax.fori_loop(0, own_x // (pack * batch), transform, 0)


def lane_group_select(stacked, count, width):
    rows = stacked.shape[0] // count
    lane = lax.broadcasted_iota(jnp.int32, (rows, LANES), 1)
    chosen = stacked[:rows]
    for i in range(1, count):
        chosen = jnp.where(lane >= i * width, stacked[i * rows : (i + 1) * rows], chosen)
    return chosen


def rolled_stack(value, count, width):
    parts = [value] + [pltpu.roll(value, d * width, 1) for d in range(1, count)]
    return jnp.concatenate(parts, axis=0) if count > 1 else value


def forward_kernel(lines_ref, cx_ref, cy_ref, plane_ref, wave_z_ref, edge_ref, spec_ref, rim_ref, *, dims):
    block, pack, own_y, rows, batch = dims

    def some(step, carry):
        mixed = []
        for q in range(batch):
            lines = lines_ref[pl.ds(step * batch + q, rows, stride=block), :]
            stack = halves(rolled_stack(lines, pack, own_y))
            mixed.append(
                lane_group_select(product((cx_ref[0], cx_ref[1]), stack, NN), pack, own_y)
            )
        for q in range(batch):
            k = step * batch + q
            spec = product(halves(mixed[q]), (cy_ref[0], cy_ref[1]), NN)
            spec_ref[k] = spec
            local = spec / (plane_ref[...] + wave_z_ref[k, 0:1, :])
            ends = dot_nt(edge_ref[...], local)
            for e in range(2):
                for i in range(pack):
                    rim_ref[e, i, pl.ds(k, 1), :] = ends[e * pack + i : e * pack + i + 1]
        return carry

    lax.fori_loop(0, block // batch, some, 0)


def backward_kernel(
    place_ref, spec_ref, rims_ref, near_ref, far_ref, cx_ref, cy_ref, plane_ref, wave_z_ref, edge_ref,
    out_ref, push_ref, *, dims
):
    block, pack, own_y, rows, batch, parts = dims
    place = place_ref[0]
    for i in range(pack):
        near, far = near_ref[i], far_ref[i]
        diagonal = 1.0 + 2.0 * near
        jumps = [rims_ref[b, 1, i] - rims_ref[b + 1, 0, i] for b in range(parts - 1)]
        ratio, value = [], []
        for j in range(parts - 1):
            pivot = diagonal if j == 0 else diagonal - far * ratio[-1]
            inverse = 1.0 / pivot
            ratio.append(far * inverse)
            value.append((jumps[j] if j == 0 else jumps[j] + far * value[-1]) * inverse)
        for j in range(parts - 3, -1, -1):
            value[j] = value[j] + ratio[j] * value[j + 1]
        left = jnp.zeros_like(near)
        right = jnp.zeros_like(near)
        for j in range(parts - 1):
            left = jnp.where(place == j + 1, value[j], left)
            right = jnp.where(place == j, -value[j], right)
        push_ref[0, i] = left
        push_ref[1, i] = right

    fill = edge_ref.shape[0] - 2 * pack

    def some(step, carry):
        solved = []
        for q in range(batch):
            k = step * batch + q
            pushes = [push_ref[e, i, pl.ds(k, 1), :] for e in range(2) for i in range(pack)]
            if fill:
                pushes.append(jnp.zeros((fill, rows), jnp.float32))
            push = jnp.concatenate(pushes, axis=0)
            spec = spec_ref[k] + dot(push.T, edge_ref[...])
            solved.append(spec / (plane_ref[...] + wave_z_ref[k, 0:1, :]))
        for q in range(batch):
            lines = product(halves(solved[q]), (cy_ref[0], cy_ref[1]), NN)
            stack = halves(rolled_stack(lines, pack, own_y))
            mixed = product((cx_ref[0], cx_ref[1]), stack, NN)
            out_ref[pl.ds(step * batch + q, rows, stride=block), :] = lane_group_select(
                mixed, pack, own_y
            )
        return carry

    lax.fori_loop(0, block // batch, some, 0)


def last_kernel(lines_ref, cosine_ref, out_ref, *, dims):
    pack, own_y, tiles, batch = dims
    groups, packs, block, _ = lines_ref.shape

    def some(step, carry):
        for q in range(batch):
            xp = step * batch + q
            lines = jnp.concatenate([lines_ref[g, xp] for g in range(groups)], axis=0)
            values = product(halves(lines.T), (cosine_ref[0], cosine_ref[1]), NN)
            for j in range(pack):
                for h in range(tiles):
                    out_ref[h, xp * pack + j] = values[
                        j * own_y : (j + 1) * own_y, h * LANES : (h + 1) * LANES
                    ]
        return carry

    lax.fori_loop(0, packs // batch, some, 0)


def per_device(surface_ids, class_map, conductivity, normals, class_table):
    width_x, width_y, width_z = surface_ids.shape
    narrow, wide, outer = lax.axis_size("gz"), lax.axis_size("gy"), lax.axis_size("gx")
    length = width_z * narrow
    groups = outer * narrow
    own_x = width_x // narrow
    pack = LANES // width_y
    block = length // groups
    tiles = length // LANES
    rows = length // pack
    planes = own_x + 2 * HALO
    limit = 60 << 20

    class_value = jnp.zeros(class_map.shape, jnp.float32)
    for index in range(class_table.shape[0]):
        class_value = jnp.where(class_map == index, class_table[index], class_value)
    root = jnp.sqrt(class_value * conductivity)

    def split(values):
        values = values.reshape(narrow, own_x, width_y, width_z // LANES, LANES)
        return values.transpose(0, 3, 1, 2, 4)

    field = jnp.stack([split(surface_ids.astype(jnp.float32)), split(root)], axis=2)
    field = lax.all_to_all(field, "gz", split_axis=0, concat_axis=0, tiled=True)
    field = field.reshape(tiles, 2, own_x, width_y, LANES)

    axes = ("gx", "gy", "gz")

    def place(x, y):
        return (x // narrow * wide + y) * narrow + x % narrow

    def fetch(values, step_x, step_y):
        pairs = []
        for x in range(groups):
            for y in range(wide):
                if 0 <= x + step_x < groups and 0 <= y + step_y < wide:
                    pairs.append((place(x, y), place(x + step_x, y + step_y)))
        return lax.ppermute(values, axes, pairs)

    x_from = {1: slice(own_x - HALO, own_x), 0: slice(None), -1: slice(0, HALO)}
    y_from = {1: slice(width_y - HALO, width_y), 0: slice(None), -1: slice(0, HALO)}

    def beside(step_x, step_y):
        piece = field[:, :, x_from[step_x], y_from[step_y]]
        if step_y:
            piece = piece.reshape(tiles, 2, -1, LANES)
        return fetch(piece, step_x, step_y)

    pieces = [field] + [
        beside(*step)
        for step in ((1, 0), (-1, 0), (0, 1), (0, -1), (1, 1), (-1, 1), (1, -1), (-1, -1))
    ]
    extent = width_y + 2 * PAD

    entries = normals.shape[1]
    table_blocks = -(-entries // LANES)
    table = jnp.pad(normals, ((0, 0), (0, table_blocks * LANES - entries)))
    table = jnp.broadcast_to(
        table.reshape(3, table_blocks, 1, LANES), (3, table_blocks, SUBLANES, LANES)
    )
    cosine = cosine_table(length)
    lines = pl.pallas_call(
        functools.partial(
            diffuse_kernel, dims=(tiles, planes, extent, own_x, width_y, pack, groups)
        ),
        out_shape=jax.ShapeDtypeStruct((groups, own_x // pack, block, LANES), jnp.float32),
        in_specs=[pl.BlockSpec(memory_space=pl.ANY)] * 3
        + [pl.BlockSpec(memory_space=pltpu.VMEM)] * 8,
        scratch_shapes=[
            pltpu.VMEM((tiles, 2, planes, extent, LANES), jnp.float32),
            pltpu.VMEM((3, tiles, planes, extent, LANES), jnp.float32),
            pltpu.VMEM((3, tiles, planes, extent, LANES), jnp.float32),
            pltpu.VMEM((tiles, planes, extent, LANES), jnp.float32),
            pltpu.VMEM((tiles, planes, extent, LANES), jnp.float32),
            pltpu.VMEM((3, tiles, width_y + 2 * SUBLANES, LANES), jnp.float32),
            pltpu.VMEM((3, tiles, width_y + 2 * SUBLANES, LANES), jnp.float32),
            pltpu.SemaphoreType.DMA((3,)),
        ],
        compiler_params=pltpu.CompilerParams(vmem_limit_bytes=limit),
        name="diffuse",
    )(*pieces, table, table_halves(cosine))
    lines = lax.all_to_all(lines, ("gx", "gz"), split_axis=0, concat_axis=0, tiled=True)

    spectra = eigen_values(length)
    screen = np.float32(4.0 / (length * length))
    local = exact_table(width_y)
    local_values = 2.0 - 2.0 * np.cos(np.pi * np.arange(width_y) / width_y)
    order_x = np.arange(rows) // (own_x // pack) * own_x + np.arange(rows) % (own_x // pack) * pack
    forward_x = np.zeros((pack, rows, pack, rows), np.float32)
    inverse_x = np.zeros((pack, rows, pack, rows), np.float32)
    for i in range(pack):
        for d in range(pack):
            other = (i - d) % pack
            forward_x[i, :, d, :] = cosine[i * rows : (i + 1) * rows][:, order_x + other]
            inverse_x[i, :, d, :] = cosine[other * rows : (other + 1) * rows][:, order_x + i].T
    forward_x = forward_x.reshape(length, length)
    inverse_x = inverse_x.reshape(length, length)
    eye = np.eye(pack)
    forward_y = np.kron(eye, -local.T).astype(np.float32)
    inverse_y = np.kron(eye, local).astype(np.float32)
    edge = np.concatenate([np.kron(eye, local[:, 0][None]), np.kron(eye, local[:, -1][None])])
    edge_rows = -(-2 * pack // SUBLANES) * SUBLANES
    edge = np.pad(edge, ((0, edge_rows - 2 * pack), (0, 0))).astype(np.float32)
    spectra_x = spectra.reshape(pack, rows)
    plane = (
        spectra_x.T[:, :, None] + local_values.astype(np.float32)[None, None, :] + screen
    ).reshape(rows, LANES)
    shift = (spectra[:, None].astype(np.float64) + spectra[None, :] + float(screen))[:, :, None]
    weights = 1.0 / (shift + local_values)
    near = (weights @ (local[:, 0] ** 2)).astype(np.float32)
    far = (weights @ (local[:, 0] * local[:, -1])).astype(np.float32)
    near = near.reshape(length, pack, rows).transpose(1, 0, 2)
    far = far.reshape(length, pack, rows).transpose(1, 0, 2)
    group = lax.axis_index("gx") * narrow + lax.axis_index("gz")
    near, far = (
        lax.dynamic_slice_in_dim(jnp.asarray(t), group * block, block, axis=1) for t in (near, far)
    )
    wave_z = lax.dynamic_slice_in_dim(jnp.asarray(spectra), group * block, block)
    wave_z = jnp.broadcast_to(wave_z[:, None, None], (block, SUBLANES, LANES))
    plane, edge = jnp.asarray(plane), jnp.asarray(edge)

    spec, rim = pl.pallas_call(
        functools.partial(forward_kernel, dims=(block, pack, width_y, rows, 4)),
        out_shape=(
            jax.ShapeDtypeStruct((block, rows, LANES), jnp.float32),
            jax.ShapeDtypeStruct((2, pack, block, rows), jnp.float32),
        ),
        name="forward",
    )(
        lines.reshape(rows * block, LANES), table_halves(forward_x), table_halves(forward_y),
        plane, wave_z, edge,
    )
    rims = lax.all_gather(rim, "gy")
    solved = pl.pallas_call(
        functools.partial(backward_kernel, dims=(block, pack, width_y, rows, 4, wide)),
        out_shape=jax.ShapeDtypeStruct((rows * block, LANES), jnp.float32),
        in_specs=[pl.BlockSpec(memory_space=pltpu.SMEM)]
        + [pl.BlockSpec(memory_space=pltpu.VMEM)] * 9,
        scratch_shapes=[pltpu.VMEM((2, pack, block, rows), jnp.float32)],
        name="backward",
    )(
        lax.axis_index("gy").reshape(1).astype(jnp.int32), spec, rims, near, far,
        table_halves(inverse_x), table_halves(inverse_y), plane, wave_z, edge,
    )
    lines = solved.reshape(groups, own_x // pack, block, LANES)
    lines = lax.all_to_all(lines, ("gx", "gz"), split_axis=0, concat_axis=0, tiled=True)
    distance = pl.pallas_call(
        functools.partial(last_kernel, dims=(pack, width_y, tiles, 2)),
        out_shape=jax.ShapeDtypeStruct((tiles, own_x, width_y, LANES), jnp.float32),
        name="last",
    )(lines, table_halves(cosine))
    distance = distance.reshape(narrow, width_z // LANES, own_x, width_y, LANES)
    distance = lax.all_to_all(distance, "gz", split_axis=0, concat_axis=0, tiled=True)
    return distance.transpose(0, 2, 3, 1, 4).reshape(width_x, width_y, width_z)


def solution(mesh):
    in_specs = (P("gx", "gy", "gz"), P("gx", "gy", "gz"), P("gx", "gy", "gz"), P(), P())
    out_specs = P("gx", "gy", "gz")
    return jax.shard_map(
        per_device, mesh=mesh, in_specs=in_specs, out_specs=out_specs, check_vma=False
    )
```

```python
import functools

import jax
import jax.numpy as jnp
import numpy as np
from jax import lax
from jax.experimental import pallas as pl
from jax.experimental.pallas import tpu as pltpu
from jax.sharding import PartitionSpec as P

STEPS = 8
TIME_STEP = 0.08
NORM_FLOOR = 0.5
LANES = 128
SUBLANES = 8
HALO = STEPS + 1
PAD = 2 * SUBLANES
HIGHEST = lax.Precision.HIGHEST


def cosine_table(length):
    f32 = np.float32
    wave = np.arange(length, dtype=f32)[:, None]
    sample = np.arange(length, dtype=f32)[None, :]
    factor = np.where(wave == 0, np.sqrt(f32(1.0 / length)), np.sqrt(f32(2.0 / length)))
    angle = f32(np.pi) * wave * (f32(2.0) * sample + f32(1.0)) / f32(2.0 * length)
    return (factor * np.cos(angle)).astype(f32)


def eigen_values(length):
    wave = np.arange(length, dtype=np.float32)
    return (np.float32(2.0) - np.float32(2.0) * np.cos(np.float32(np.pi) * wave / np.float32(length))).astype(
        np.float32
    )


def exact_table(length):
    wave = np.arange(length, dtype=np.float64)[:, None]
    sample = np.arange(length, dtype=np.float64)[None, :]
    factor = np.where(wave == 0, np.sqrt(1.0 / length), np.sqrt(2.0 / length))
    return factor * np.cos(np.pi * wave * (2.0 * sample + 1.0) / (2.0 * length))


def dot(a, b):
    return jnp.dot(a, b, precision=HIGHEST, preferred_element_type=jnp.float32)


def dot_nt(a, b):
    return lax.dot_general(
        a, b, (((1,), (1,)), ((), ())), precision=HIGHEST, preferred_element_type=jnp.float32
    )


def halves(values):
    high = values.astype(jnp.bfloat16)
    return high, (values - high.astype(jnp.float32)).astype(jnp.bfloat16)


def table_halves(table):
    table = np.asarray(table, np.float32)
    high = table.astype(jnp.bfloat16)
    return jnp.asarray(np.stack([high, (table - high.astype(np.float32)).astype(jnp.bfloat16)]))


def product(a, b, contract):
    def part(x, y):
        return lax.dot_general(x, y, (contract, ((), ())), preferred_element_type=jnp.float32)

    return part(a[0], b[0]) + (part(a[0], b[1]) + part(a[1], b[0]))


NN = ((1,), (0,))
NT = ((1,), (1,))


def z_neighbours(tiles, first, last):
    above = jnp.where(last, 0.0, pltpu.roll(tiles[0], LANES - 1, 1))
    below = jnp.where(first, 0.0, pltpu.roll(tiles[-1], 1, 1))
    return [*tiles[1:], above], [below, *tiles[:-1]]


def diffuse_kernel(
    own_ref, west_ref, east_ref, south_ref, north_ref, sw_ref, se_ref, nw_ref, ne_ref, table_ref, order_ref, cosine_ref,
    out_ref, field_ref, va, vb, keep_ref, gain_ref, za, zb, sems, *, dims
):
    tiles, planes, rows, own_x, own_y, pack, groups = dims
    span = own_y + 2 * SUBLANES
    chunk = pl.ds(SUBLANES, span)
    lane = lax.broadcasted_iota(jnp.int32, (span, LANES), 1)
    first, last = lane == 0, lane == LANES - 1
    table_blocks = table_ref.shape[1]
    every = range(tiles)
    own_rows = pl.ds(PAD, own_y)

    copies = [
        pltpu.make_async_copy(
            ref, field_ref.at[:, :, pl.ds(start, size), own_rows, :], sems.at[n]
        )
        for n, (ref, start, size) in enumerate(
            ((west_ref, 0, HALO), (own_ref, HALO, own_x), (east_ref, HALO + own_x, HALO))
        )
    ]
    for copy in copies:
        copy.start()

    def rim(ref, begin, above):
        def one(x, carry):
            for h in every:
                for f in range(2):
                    if above:
                        eight, single, at = x * HALO, x * HALO + SUBLANES, PAD + own_y
                        far = at + SUBLANES
                    else:
                        eight, single, at = x * HALO + 1, x * HALO, SUBLANES
                        far = at - 1
                    field_ref[h, f, begin + x, pl.ds(at, SUBLANES), :] = ref[
                        h, f, pl.ds(eight, SUBLANES), :
                    ]
                    field_ref[h, f, begin + x, pl.ds(far, 1), :] = ref[h, f, pl.ds(single, 1), :]
            return carry

        lax.fori_loop(0, ref.shape[2] // HALO, one, 0)

    rim(sw_ref, 0, False)
    rim(south_ref, HALO, False)
    rim(se_ref, HALO + own_x, False)
    rim(nw_ref, 0, True)
    rim(north_ref, HALO, True)
    rim(ne_ref, HALO + own_x, True)
    for copy in copies:
        copy.wait()

    used = pl.ds(0, span + 2 * SUBLANES)

    def reorder(x, carry):
        for f, parts in ((0, 1 if table_blocks * LANES <= 256 else 2), (1, 3)):
            rest = jnp.concatenate([field_ref[h, f, x, used, :] for h in every], axis=1)
            moved = None
            for _ in range(parts):
                part = rest.astype(jnp.bfloat16)
                rest = rest - part.astype(jnp.float32)
                picked = jnp.dot(part, order_ref[...], preferred_element_type=jnp.float32)
                moved = picked if moved is None else moved + picked
            for h in every:
                field_ref[h, f, x, used, :] = moved[:, h * LANES : (h + 1) * LANES]
        return carry

    lax.fori_loop(0, planes, reorder, 0)

    row = lax.broadcasted_iota(jnp.int32, (SUBLANES, LANES), 0)

    def spread(x):
        for y in range(span // SUBLANES + 2):
            at = pl.ds(y * SUBLANES, SUBLANES)
            for h in every:
                ids = field_ref[h, 0, x, at, :]
                root = field_ref[h, 1, x, at, :]
                if y == 0 or y == span // SUBLANES + 1:
                    inside = row == (SUBLANES - 1 if y == 0 else 0)
                    ids = jnp.where(inside, ids, 0.0)
                    root = jnp.where(inside, root, 0.0)
                ids = ids.astype(jnp.int32)
                low = (ids - 1) & (LANES - 1)
                high = (ids - 1) >> (LANES.bit_length() - 1)
                for c in range(3):
                    value = jnp.zeros((SUBLANES, LANES), jnp.float32)
                    for k in range(table_blocks):
                        found = jnp.take_along_axis(table_ref[c, k], low, axis=1)
                        value = jnp.where(high == k, found, value)
                    va[c, h, x, at, :] = value * root

    def coefficients(x):
        one = jnp.minimum(x, 1)
        mid = [field_ref[h, 1, x, chunk, :] for h in every]
        up, down = z_neighbours(mid, first, last)
        for h in every:
            total = (
                (field_ref[h, 1, x + 1, chunk, :] + field_ref[h, 1, x - 1, chunk, :])
                + (
                    field_ref[h, 1, x, pl.ds(SUBLANES + one, span), :]
                    + field_ref[h, 1, x, pl.ds(SUBLANES - one, span), :]
                )
                + (up[h] + down[h])
            )
            scaled = TIME_STEP * mid[h]
            keep_ref[h, x, chunk, :] = 1.0 - scaled * total
            gain_ref[h, x, chunk, :] = scaled * mid[h]

    def prepare(x, carry):
        spread(x)
        coefficients(x)
        return carry

    spread(0)
    lax.fori_loop(1, planes - 1, prepare, 0)
    spread(planes - 1)

    tile_lane = lax.broadcasted_iota(jnp.int32, (SUBLANES, LANES), 1)
    tile_first, tile_last = tile_lane == 0, tile_lane == LANES - 1

    def along_z(source, x, y, kept):
        at = pl.ds(SUBLANES * (y + 1), SUBLANES)
        for c in range(3):
            up, down = z_neighbours([source[c, h, x, at, :] for h in every], tile_first, tile_last)
            for h in every:
                kept[c, h, pl.ds(y * SUBLANES, SUBLANES), :] = up[h] + down[h]

    def update(source, target, x, y, one):
        base = SUBLANES * (y + 1)
        at = pl.ds(base, SUBLANES)
        for h in every:
            keep = [keep_ref[h, x + i, at, :] for i in range(2)]
            gain = [gain_ref[h, x + i, at, :] for i in range(2)]
            for c in range(3):
                line = [source[c, h, x + i, at, :] for i in range(-1, 3)]
                for i, kept in enumerate((za, zb)):
                    total = (
                        (line[i] + line[i + 2])
                        + (
                            source[c, h, x + i, pl.ds(base + one, SUBLANES), :]
                            + source[c, h, x + i, pl.ds(base - one, SUBLANES), :]
                        )
                        + kept[c, h, pl.ds(y * SUBLANES, SUBLANES), :]
                    )
                    target[c, h, x + i, at, :] = keep[i] * line[i + 1] + gain[i] * total

    def sweep(source, target, begin):
        for y in range(span // SUBLANES):
            along_z(source, begin, y, za)
            along_z(source, begin + 1, y, zb)

        def two_planes(pair, carry):
            x = begin + 2 * pair
            one = jnp.minimum(x, 1)
            ahead = jnp.minimum(x + 3, planes - 1)
            for y in range(span // SUBLANES):
                update(source, target, x, y, one)
                along_z(source, x + 2, y, za)
                along_z(source, ahead, y, zb)
            return carry

        lax.fori_loop(0, planes // 2 - begin, two_planes, 0)

    def two_steps(pair, carry):
        sweep(va, vb, 2 * pair + 1)
        sweep(vb, va, 2 * pair + 2)
        return carry

    lax.fori_loop(0, STEPS // 2, two_steps, 0)

    def unit(x, carry):
        for h in every:
            root = field_ref[h, 1, x, chunk, :]
            inverse = jnp.where(root > 0.0, 1.0 / jnp.where(root > 0.0, root, 1.0), 0.0)
            heat = [va[c, h, x, chunk, :] * inverse for c in range(3)]
            size = jnp.sqrt(heat[0] * heat[0] + heat[1] * heat[1] + heat[2] * heat[2])
            scale = 0.5 / jnp.maximum(size, NORM_FLOOR)
            for c in range(3):
                vb[c, h, x, chunk, :] = heat[c] * scale
        return carry

    lax.fori_loop(STEPS, planes - STEPS, unit, 0)

    own_lane = lax.broadcasted_iota(jnp.int32, (own_y, LANES), 1)
    own_first, own_last = own_lane == 0, own_lane == LANES - 1
    block = out_ref.shape[2]
    batch = 2

    def transform(step, carry):
        one = jnp.minimum(step + 1, 1)
        slabs = []
        for j in range(batch * pack):
            x = HALO + step * (batch * pack) + j
            up, down = z_neighbours([vb[2, h, x, own_rows, :] for h in every], own_first, own_last)
            slabs.append(
                jnp.concatenate(
                    [
                        (vb[0, h, x + 1, own_rows, :] - vb[0, h, x - 1, own_rows, :])
                        + (
                            vb[1, h, x, pl.ds(PAD + one, own_y), :]
                            - vb[1, h, x, pl.ds(PAD - one, own_y), :]
                        )
                        + (up[h] - down[h])
                        for h in every
                    ],
                    axis=1,
                )
            )
        lines = halves(jnp.concatenate(slabs, axis=0))
        spectrum = product((cosine_ref[0], cosine_ref[1]), lines, NT)
        for q in range(batch):
            for g in range(groups):
                out_ref[g, step * batch + q] = spectrum[
                    g * block : (g + 1) * block, q * LANES : (q + 1) * LANES
                ]
        return carry

    lax.fori_loop(0, own_x // (pack * batch), transform, 0)


def lane_group_select(stacked, count, width):
    rows = stacked.shape[0] // count
    lane = lax.broadcasted_iota(jnp.int32, (rows, LANES), 1)
    chosen = stacked[:rows]
    for i in range(1, count):
        chosen = jnp.where(lane >= i * width, stacked[i * rows : (i + 1) * rows], chosen)
    return chosen


def rolled_stack(value, count, width):
    parts = [value] + [pltpu.roll(value, d * width, 1) for d in range(1, count)]
    return jnp.concatenate(parts, axis=0) if count > 1 else value


def forward_kernel(lines_ref, cx_ref, cy_ref, plane_ref, wave_z_ref, edge_ref, spec_ref, rim_ref, *, dims):
    block, pack, own_y, rows, batch = dims

    def some(step, carry):
        mixed = []
        for q in range(batch):
            lines = lines_ref[pl.ds(step * batch + q, rows, stride=block), :]
            stack = halves(rolled_stack(lines, pack, own_y))
            mixed.append(
                lane_group_select(product((cx_ref[0], cx_ref[1]), stack, NN), pack, own_y)
            )
        for q in range(batch):
            k = step * batch + q
            spec = product(halves(mixed[q]), (cy_ref[0], cy_ref[1]), NN)
            spec_ref[k] = spec
            local = spec / (plane_ref[...] + wave_z_ref[k, 0:1, :])
            ends = dot_nt(edge_ref[...], local)
            for e in range(2):
                for i in range(pack):
                    rim_ref[e, i, pl.ds(k, 1), :] = ends[e * pack + i : e * pack + i + 1]
        return carry

    lax.fori_loop(0, block // batch, some, 0)


def backward_kernel(
    place_ref, spec_ref, rims_ref, near_ref, far_ref, cx_ref, cy_ref, plane_ref, wave_z_ref, edge_ref,
    out_ref, push_ref, *, dims
):
    block, pack, own_y, rows, batch, parts = dims
    place = place_ref[0]
    for i in range(pack):
        near, far = near_ref[i], far_ref[i]
        diagonal = 1.0 + 2.0 * near
        at = [(place + (parts - b)) % parts for b in range(parts)]
        jumps = [rims_ref[at[b], 1, i] - rims_ref[at[b + 1], 0, i] for b in range(parts - 1)]
        ratio, value = [], []
        for j in range(parts - 1):
            pivot = diagonal if j == 0 else diagonal - far * ratio[-1]
            inverse = 1.0 / pivot
            ratio.append(far * inverse)
            value.append((jumps[j] if j == 0 else jumps[j] + far * value[-1]) * inverse)
        for j in range(parts - 3, -1, -1):
            value[j] = value[j] + ratio[j] * value[j + 1]
        left = jnp.zeros_like(near)
        right = jnp.zeros_like(near)
        for j in range(parts - 1):
            left = jnp.where(place == j + 1, value[j], left)
            right = jnp.where(place == j, -value[j], right)
        push_ref[0, i] = left
        push_ref[1, i] = right

    fill = edge_ref.shape[0] - 2 * pack

    def some(step, carry):
        solved = []
        for q in range(batch):
            k = step * batch + q
            pushes = [push_ref[e, i, pl.ds(k, 1), :] for e in range(2) for i in range(pack)]
            if fill:
                pushes.append(jnp.zeros((fill, rows), jnp.float32))
            push = jnp.concatenate(pushes, axis=0)
            spec = spec_ref[k] + dot(push.T, edge_ref[...])
            solved.append(spec / (plane_ref[...] + wave_z_ref[k, 0:1, :]))
        for q in range(batch):
            lines = product(halves(solved[q]), (cy_ref[0], cy_ref[1]), NN)
            stack = halves(rolled_stack(lines, pack, own_y))
            mixed = product((cx_ref[0], cx_ref[1]), stack, NN)
            out_ref[pl.ds(step * batch + q, rows, stride=block), :] = lane_group_select(
                mixed, pack, own_y
            )
        return carry

    lax.fori_loop(0, block // batch, some, 0)


def last_kernel(lines_ref, cosine_ref, out_ref, *, dims):
    pack, own_y, tiles, batch = dims
    groups, packs, block, _ = lines_ref.shape

    def some(step, carry):
        for q in range(batch):
            xp = step * batch + q
            lines = jnp.concatenate([lines_ref[g, xp] for g in range(groups)], axis=0)
            values = product(halves(lines.T), (cosine_ref[0], cosine_ref[1]), NN)
            for j in range(pack):
                for h in range(tiles):
                    out_ref[h, xp * pack + j] = values[
                        j * own_y : (j + 1) * own_y, h * LANES : (h + 1) * LANES
                    ]
        return carry

    lax.fori_loop(0, packs // batch, some, 0)


def per_device(surface_ids, class_map, conductivity, normals, class_table):
    width_x, width_y, width_z = surface_ids.shape
    narrow, wide, outer = lax.axis_size("gz"), lax.axis_size("gy"), lax.axis_size("gx")
    length = width_z * narrow
    groups = outer * narrow
    own_x = width_x // narrow
    pack = LANES // width_y
    block = length // groups
    tiles = length // LANES
    rows = length // pack
    planes = own_x + 2 * HALO
    limit = 60 << 20

    class_value = jnp.zeros(class_map.shape, jnp.float32)
    for index in range(class_table.shape[0]):
        class_value = jnp.where(class_map == index, class_table[index], class_value)
    root = jnp.sqrt(class_value * conductivity)

    def split(values):
        values = values.reshape(narrow, own_x, width_y, width_z // LANES, LANES)
        return values.transpose(0, 3, 1, 2, 4)

    field = jnp.stack([split(surface_ids.astype(jnp.float32)), split(root)], axis=2)
    field = lax.all_to_all(field, "gz", split_axis=0, concat_axis=0, tiled=True)
    field = field.reshape(tiles, 2, own_x, width_y, LANES)

    axes = ("gx", "gy", "gz")

    def place(x, y):
        return (x // narrow * wide + y) * narrow + x % narrow

    def fetch(values, step_x, step_y):
        pairs = []
        for x in range(groups):
            for y in range(wide):
                if 0 <= x + step_x < groups and 0 <= y + step_y < wide:
                    pairs.append((place(x, y), place(x + step_x, y + step_y)))
        return lax.ppermute(values, axes, pairs)

    x_from = {1: slice(own_x - HALO, own_x), 0: slice(None), -1: slice(0, HALO)}
    y_from = {1: slice(width_y - HALO, width_y), 0: slice(None), -1: slice(0, HALO)}

    def beside(step_x, step_y):
        piece = field[:, :, x_from[step_x], y_from[step_y]]
        if step_y:
            piece = piece.reshape(tiles, 2, -1, LANES)
        return fetch(piece, step_x, step_y)

    pieces = [field] + [
        beside(*step)
        for step in ((1, 0), (-1, 0), (0, 1), (0, -1), (1, 1), (-1, 1), (1, -1), (-1, -1))
    ]
    extent = width_y + 2 * PAD + SUBLANES

    entries = normals.shape[1]
    table_blocks = -(-entries // LANES)
    table = jnp.pad(normals, ((0, 0), (0, table_blocks * LANES - entries)))
    table = jnp.broadcast_to(
        table.reshape(3, table_blocks, 1, LANES), (3, table_blocks, SUBLANES, LANES)
    )
    cosine = cosine_table(length)
    cells = np.arange(length) % LANES * tiles + np.arange(length) // LANES
    order = np.arange(length)[:, None] == cells[None, :]
    lines = pl.pallas_call(
        functools.partial(
            diffuse_kernel, dims=(tiles, planes, extent, own_x, width_y, pack, groups)
        ),
        out_shape=jax.ShapeDtypeStruct((groups, own_x // pack, block, LANES), jnp.float32),
        in_specs=[pl.BlockSpec(memory_space=pl.ANY)] * 3
        + [pl.BlockSpec(memory_space=pltpu.VMEM)] * 9,
        scratch_shapes=[
            pltpu.VMEM((tiles, 2, planes, extent, LANES), jnp.float32),
            pltpu.VMEM((3, tiles, planes, extent, LANES), jnp.float32),
            pltpu.VMEM((3, tiles, planes, extent, LANES), jnp.float32),
            pltpu.VMEM((tiles, planes, extent, LANES), jnp.float32),
            pltpu.VMEM((tiles, planes, extent, LANES), jnp.float32),
            pltpu.VMEM((3, tiles, width_y + 2 * SUBLANES, LANES), jnp.float32),
            pltpu.VMEM((3, tiles, width_y + 2 * SUBLANES, LANES), jnp.float32),
            pltpu.SemaphoreType.DMA((3,)),
        ],
        compiler_params=pltpu.CompilerParams(vmem_limit_bytes=limit),
        name="diffuse",
    )(*pieces, table, jnp.asarray(order.astype(jnp.bfloat16)), table_halves(cosine[:, cells]))
    lines = lax.all_to_all(lines, ("gx", "gz"), split_axis=0, concat_axis=0, tiled=True)

    spectra = eigen_values(length)
    screen = np.float32(4.0 / (length * length))
    local = exact_table(width_y)
    local_values = 2.0 - 2.0 * np.cos(np.pi * np.arange(width_y) / width_y)
    order_x = np.arange(rows) // (own_x // pack) * own_x + np.arange(rows) % (own_x // pack) * pack
    forward_x = np.zeros((pack, rows, pack, rows), np.float32)
    inverse_x = np.zeros((pack, rows, pack, rows), np.float32)
    for i in range(pack):
        for d in range(pack):
            other = (i - d) % pack
            forward_x[i, :, d, :] = cosine[i * rows : (i + 1) * rows][:, order_x + other]
            inverse_x[i, :, d, :] = cosine[other * rows : (other + 1) * rows][:, order_x + i].T
    forward_x = forward_x.reshape(length, length)
    inverse_x = inverse_x.reshape(length, length)
    eye = np.eye(pack)
    forward_y = np.kron(eye, -local.T).astype(np.float32)
    inverse_y = np.kron(eye, local).astype(np.float32)
    edge = np.concatenate([np.kron(eye, local[:, 0][None]), np.kron(eye, local[:, -1][None])])
    edge_rows = -(-2 * pack // SUBLANES) * SUBLANES
    edge = np.pad(edge, ((0, edge_rows - 2 * pack), (0, 0))).astype(np.float32)
    spectra_x = spectra.reshape(pack, rows)
    plane = (
        spectra_x.T[:, :, None] + local_values.astype(np.float32)[None, None, :] + screen
    ).reshape(rows, LANES)
    shift = (spectra[:, None].astype(np.float64) + spectra[None, :] + float(screen))[:, :, None]
    weights = 1.0 / (shift + local_values)
    near = (weights @ (local[:, 0] ** 2)).astype(np.float32)
    far = (weights @ (local[:, 0] * local[:, -1])).astype(np.float32)
    near = near.reshape(length, pack, rows).transpose(1, 0, 2)
    far = far.reshape(length, pack, rows).transpose(1, 0, 2)
    group = lax.axis_index("gx") * narrow + lax.axis_index("gz")
    near, far = (
        lax.dynamic_slice_in_dim(jnp.asarray(t), group * block, block, axis=1) for t in (near, far)
    )
    wave_z = lax.dynamic_slice_in_dim(jnp.asarray(spectra), group * block, block)
    wave_z = jnp.broadcast_to(wave_z[:, None, None], (block, SUBLANES, LANES))
    plane, edge = jnp.asarray(plane), jnp.asarray(edge)

    spec, rim = pl.pallas_call(
        functools.partial(forward_kernel, dims=(block, pack, width_y, rows, 4)),
        out_shape=(
            jax.ShapeDtypeStruct((block, rows, LANES), jnp.float32),
            jax.ShapeDtypeStruct((2, pack, block, rows), jnp.float32),
        ),
        name="forward",
    )(
        lines.reshape(rows * block, LANES), table_halves(forward_x), table_halves(forward_y),
        plane, wave_z, edge,
    )
    rims = jnp.stack(
        [rim]
        + [
            lax.ppermute(rim, "gy", [(i, (i + step) % wide) for i in range(wide)])
            for step in range(1, wide)
        ]
    )
    solved = pl.pallas_call(
        functools.partial(backward_kernel, dims=(block, pack, width_y, rows, 4, wide)),
        out_shape=jax.ShapeDtypeStruct((rows * block, LANES), jnp.float32),
        in_specs=[pl.BlockSpec(memory_space=pltpu.SMEM)]
        + [pl.BlockSpec(memory_space=pltpu.VMEM)] * 9,
        scratch_shapes=[pltpu.VMEM((2, pack, block, rows), jnp.float32)],
        name="backward",
    )(
        lax.axis_index("gy").reshape(1).astype(jnp.int32), spec, rims, near, far,
        table_halves(inverse_x), table_halves(inverse_y), plane, wave_z, edge,
    )
    lines = solved.reshape(groups, own_x // pack, block, LANES)
    lines = lax.all_to_all(lines, ("gx", "gz"), split_axis=0, concat_axis=0, tiled=True)
    distance = pl.pallas_call(
        functools.partial(last_kernel, dims=(pack, width_y, tiles, 2)),
        out_shape=jax.ShapeDtypeStruct((tiles, own_x, width_y, LANES), jnp.float32),
        name="last",
    )(lines, table_halves(cosine))
    distance = distance.reshape(narrow, width_z // LANES, own_x, width_y, LANES)
    distance = lax.all_to_all(distance, "gz", split_axis=0, concat_axis=0, tiled=True)
    return distance.transpose(0, 2, 3, 1, 4).reshape(width_x, width_y, width_z)


def solution(mesh):
    in_specs = (P("gx", "gy", "gz"), P("gx", "gy", "gz"), P("gx", "gy", "gz"), P(), P())
    out_specs = P("gx", "gy", "gz")
    return jax.shard_map(
        per_device, mesh=mesh, in_specs=in_specs, out_specs=out_specs, check_vma=False
    )
```

```python
import functools

import jax
import jax.numpy as jnp
import numpy as np
from jax import lax
from jax.experimental import pallas as pl
from jax.experimental.pallas import tpu as pltpu
from jax.sharding import PartitionSpec as P

STEPS = 8
TIME_STEP = 0.08
NORM_FLOOR = 0.5
LANES = 128
SUBLANES = 8
HALO = STEPS + 1
PAD = 2 * SUBLANES
HIGHEST = lax.Precision.HIGHEST


def cosine_table(length):
    f32 = np.float32
    wave = np.arange(length, dtype=f32)[:, None]
    sample = np.arange(length, dtype=f32)[None, :]
    factor = np.where(wave == 0, np.sqrt(f32(1.0 / length)), np.sqrt(f32(2.0 / length)))
    angle = f32(np.pi) * wave * (f32(2.0) * sample + f32(1.0)) / f32(2.0 * length)
    return (factor * np.cos(angle)).astype(f32)


def eigen_values(length):
    wave = np.arange(length, dtype=np.float32)
    return (np.float32(2.0) - np.float32(2.0) * np.cos(np.float32(np.pi) * wave / np.float32(length))).astype(
        np.float32
    )


def exact_table(length):
    wave = np.arange(length, dtype=np.float64)[:, None]
    sample = np.arange(length, dtype=np.float64)[None, :]
    factor = np.where(wave == 0, np.sqrt(1.0 / length), np.sqrt(2.0 / length))
    return factor * np.cos(np.pi * wave * (2.0 * sample + 1.0) / (2.0 * length))


def dot(a, b):
    return jnp.dot(a, b, precision=HIGHEST, preferred_element_type=jnp.float32)


def dot_nt(a, b):
    return lax.dot_general(
        a, b, (((1,), (1,)), ((), ())), precision=HIGHEST, preferred_element_type=jnp.float32
    )


def halves(values):
    high = values.astype(jnp.bfloat16)
    return high, (values - high.astype(jnp.float32)).astype(jnp.bfloat16)


def table_halves(table):
    table = np.asarray(table, np.float32)
    high = table.astype(jnp.bfloat16)
    return jnp.asarray(np.stack([high, (table - high.astype(np.float32)).astype(jnp.bfloat16)]))


def product(a, b, contract):
    def part(x, y):
        return lax.dot_general(x, y, (contract, ((), ())), preferred_element_type=jnp.float32)

    return part(a[0], b[0]) + (part(a[0], b[1]) + part(a[1], b[0]))


NN = ((1,), (0,))
NT = ((1,), (1,))


def z_neighbours(tiles, first, last):
    above = jnp.where(last, 0.0, pltpu.roll(tiles[0], LANES - 1, 1))
    below = jnp.where(first, 0.0, pltpu.roll(tiles[-1], 1, 1))
    return [*tiles[1:], above], [below, *tiles[:-1]]


def diffuse_kernel(
    own_ref, west_ref, east_ref, south_ref, north_ref, sw_ref, se_ref, nw_ref, ne_ref, table_ref, order_ref, cosine_ref,
    out_ref, late_ref, field_ref, va, vb, keep_ref, gain_ref, za, zb, sems, *, dims
):
    tiles, planes, rows, own_x, own_y, pack, groups = dims
    span = own_y + 2 * SUBLANES
    chunk = pl.ds(SUBLANES, span)
    lane = lax.broadcasted_iota(jnp.int32, (span, LANES), 1)
    first, last = lane == 0, lane == LANES - 1
    table_blocks = table_ref.shape[1]
    every = range(tiles)
    own_rows = pl.ds(PAD, own_y)

    copies = [
        pltpu.make_async_copy(
            ref, field_ref.at[:, :, pl.ds(start, size), own_rows, :], sems.at[n]
        )
        for n, (ref, start, size) in enumerate(
            ((west_ref, 0, HALO), (own_ref, HALO, own_x), (east_ref, HALO + own_x, HALO))
        )
    ]
    for copy in copies:
        copy.start()

    def rim(ref, begin, above):
        def one(x, carry):
            for h in every:
                for f in range(2):
                    if above:
                        eight, single, at = x * HALO, x * HALO + SUBLANES, PAD + own_y
                        far = at + SUBLANES
                    else:
                        eight, single, at = x * HALO + 1, x * HALO, SUBLANES
                        far = at - 1
                    field_ref[h, f, begin + x, pl.ds(at, SUBLANES), :] = ref[
                        h, f, pl.ds(eight, SUBLANES), :
                    ]
                    field_ref[h, f, begin + x, pl.ds(far, 1), :] = ref[h, f, pl.ds(single, 1), :]
            return carry

        lax.fori_loop(0, ref.shape[2] // HALO, one, 0)

    rim(sw_ref, 0, False)
    rim(south_ref, HALO, False)
    rim(se_ref, HALO + own_x, False)
    rim(nw_ref, 0, True)
    rim(north_ref, HALO, True)
    rim(ne_ref, HALO + own_x, True)
    for copy in copies:
        copy.wait()

    used = pl.ds(0, span + 2 * SUBLANES)

    def reorder(x, carry):
        for f, parts in ((0, 1 if table_blocks * LANES <= 256 else 2), (1, 3)):
            rest = jnp.concatenate([field_ref[h, f, x, used, :] for h in every], axis=1)
            moved = None
            for _ in range(parts):
                part = rest.astype(jnp.bfloat16)
                rest = rest - part.astype(jnp.float32)
                picked = jnp.dot(part, order_ref[...], preferred_element_type=jnp.float32)
                moved = picked if moved is None else moved + picked
            for h in every:
                field_ref[h, f, x, used, :] = moved[:, h * LANES : (h + 1) * LANES]
        return carry

    lax.fori_loop(0, planes, reorder, 0)

    row = lax.broadcasted_iota(jnp.int32, (SUBLANES, LANES), 0)

    def spread(x):
        for y in range(span // SUBLANES + 2):
            at = pl.ds(y * SUBLANES, SUBLANES)
            for h in every:
                ids = field_ref[h, 0, x, at, :]
                root = field_ref[h, 1, x, at, :]
                if y == 0 or y == span // SUBLANES + 1:
                    inside = row == (SUBLANES - 1 if y == 0 else 0)
                    ids = jnp.where(inside, ids, 0.0)
                    root = jnp.where(inside, root, 0.0)
                ids = ids.astype(jnp.int32)
                low = (ids - 1) & (LANES - 1)
                high = (ids - 1) >> (LANES.bit_length() - 1)
                for c in range(3):
                    value = jnp.zeros((SUBLANES, LANES), jnp.float32)
                    for k in range(table_blocks):
                        found = jnp.take_along_axis(table_ref[c, k], low, axis=1)
                        value = jnp.where(high == k, found, value)
                    va[c, h, x, at, :] = value * root

    def coefficients(x):
        one = jnp.minimum(x, 1)
        mid = [field_ref[h, 1, x, chunk, :] for h in every]
        up, down = z_neighbours(mid, first, last)
        for h in every:
            total = (
                (field_ref[h, 1, x + 1, chunk, :] + field_ref[h, 1, x - 1, chunk, :])
                + (
                    field_ref[h, 1, x, pl.ds(SUBLANES + one, span), :]
                    + field_ref[h, 1, x, pl.ds(SUBLANES - one, span), :]
                )
                + (up[h] + down[h])
            )
            scaled = TIME_STEP * mid[h]
            keep_ref[h, x, chunk, :] = 1.0 - scaled * total
            gain_ref[h, x, chunk, :] = scaled * mid[h]

    def prepare(x, carry):
        spread(x)
        coefficients(x)
        return carry

    spread(0)
    lax.fori_loop(1, planes - 1, prepare, 0)
    spread(planes - 1)

    tile_lane = lax.broadcasted_iota(jnp.int32, (SUBLANES, LANES), 1)
    tile_first, tile_last = tile_lane == 0, tile_lane == LANES - 1

    def along_z(source, x, y, kept):
        at = pl.ds(SUBLANES * (y + 1), SUBLANES)
        for c in range(3):
            up, down = z_neighbours([source[c, h, x, at, :] for h in every], tile_first, tile_last)
            for h in every:
                kept[c, h, pl.ds(y * SUBLANES, SUBLANES), :] = up[h] + down[h]

    def update(source, target, x, y, one):
        base = SUBLANES * (y + 1)
        at = pl.ds(base, SUBLANES)
        for h in every:
            keep = [keep_ref[h, x + i, at, :] for i in range(2)]
            gain = [gain_ref[h, x + i, at, :] for i in range(2)]
            for c in range(3):
                line = [source[c, h, x + i, at, :] for i in range(-1, 3)]
                for i, kept in enumerate((za, zb)):
                    total = (
                        (line[i] + line[i + 2])
                        + (
                            source[c, h, x + i, pl.ds(base + one, SUBLANES), :]
                            + source[c, h, x + i, pl.ds(base - one, SUBLANES), :]
                        )
                        + kept[c, h, pl.ds(y * SUBLANES, SUBLANES), :]
                    )
                    target[c, h, x + i, at, :] = keep[i] * line[i + 1] + gain[i] * total

    def sweep(source, target, begin):
        for y in range(span // SUBLANES):
            along_z(source, begin, y, za)
            along_z(source, begin + 1, y, zb)

        def two_planes(pair, carry):
            x = begin + 2 * pair
            one = jnp.minimum(x, 1)
            ahead = jnp.minimum(x + 3, planes - 1)
            for y in range(span // SUBLANES):
                update(source, target, x, y, one)
                along_z(source, x + 2, y, za)
                along_z(source, ahead, y, zb)
            return carry

        lax.fori_loop(0, planes // 2 - begin, two_planes, 0)

    def two_steps(pair, carry):
        sweep(va, vb, 2 * pair + 1)
        sweep(vb, va, 2 * pair + 2)
        return carry

    lax.fori_loop(0, STEPS // 2, two_steps, 0)

    def unit(x, carry):
        for h in every:
            root = field_ref[h, 1, x, chunk, :]
            inverse = jnp.where(root > 0.0, 1.0 / jnp.where(root > 0.0, root, 1.0), 0.0)
            heat = [va[c, h, x, chunk, :] * inverse for c in range(3)]
            size = jnp.sqrt(heat[0] * heat[0] + heat[1] * heat[1] + heat[2] * heat[2])
            scale = 0.5 / jnp.maximum(size, NORM_FLOOR)
            for c in range(3):
                vb[c, h, x, chunk, :] = heat[c] * scale
        return carry

    lax.fori_loop(STEPS, planes - STEPS, unit, 0)

    own_lane = lax.broadcasted_iota(jnp.int32, (own_y, LANES), 1)
    own_first, own_last = own_lane == 0, own_lane == LANES - 1
    block = out_ref.shape[2]
    batch = 2

    def transform(step, carry):
        one = jnp.minimum(step + 1, 1)
        slabs = []
        for j in range(batch * pack):
            x = HALO + step * (batch * pack) + j
            up, down = z_neighbours([vb[2, h, x, own_rows, :] for h in every], own_first, own_last)
            slabs.append(
                jnp.concatenate(
                    [
                        (vb[0, h, x + 1, own_rows, :] - vb[0, h, x - 1, own_rows, :])
                        + (
                            vb[1, h, x, pl.ds(PAD + one, own_y), :]
                            - vb[1, h, x, pl.ds(PAD - one, own_y), :]
                        )
                        + (up[h] - down[h])
                        for h in every
                    ],
                    axis=1,
                )
            )
        lines = halves(jnp.concatenate(slabs, axis=0))
        spectrum = product((cosine_ref[0], cosine_ref[1]), lines, NT)
        for q in range(batch):
            for g in range(groups):
                for n, ref in enumerate((out_ref, late_ref)):
                    begin = (2 * g + n) * block
                    ref[g, step * batch + q] = spectrum[
                        begin : begin + block, q * LANES : (q + 1) * LANES
                    ]
        return carry

    lax.fori_loop(0, own_x // (pack * batch), transform, 0)


def lane_group_select(stacked, count, width):
    rows = stacked.shape[0] // count
    lane = lax.broadcasted_iota(jnp.int32, (rows, LANES), 1)
    chosen = stacked[:rows]
    for i in range(1, count):
        chosen = jnp.where(lane >= i * width, stacked[i * rows : (i + 1) * rows], chosen)
    return chosen


def rolled_stack(value, count, width):
    parts = [value] + [pltpu.roll(value, d * width, 1) for d in range(1, count)]
    return jnp.concatenate(parts, axis=0) if count > 1 else value


def forward_kernel(lines_ref, cx_ref, cy_ref, plane_ref, wave_z_ref, edge_ref, spec_ref, rim_ref, *, dims):
    block, pack, own_y, rows, batch = dims

    def some(step, carry):
        mixed = []
        for q in range(batch):
            lines = lines_ref[pl.ds(step * batch + q, rows, stride=block), :]
            stack = halves(rolled_stack(lines, pack, own_y))
            mixed.append(
                lane_group_select(product((cx_ref[0], cx_ref[1]), stack, NN), pack, own_y)
            )
        for q in range(batch):
            k = step * batch + q
            spec = product(halves(mixed[q]), (cy_ref[0], cy_ref[1]), NN)
            spec_ref[k] = spec
            local = spec / (plane_ref[...] + wave_z_ref[k, 0:1, :])
            ends = dot_nt(edge_ref[...], local)
            for e in range(2):
                for i in range(pack):
                    rim_ref[e, i, pl.ds(k, 1), :] = ends[e * pack + i : e * pack + i + 1]
        return carry

    lax.fori_loop(0, block // batch, some, 0)


def backward_kernel(
    place_ref, spec_ref, rims_ref, near_ref, far_ref, cx_ref, cy_ref, plane_ref, wave_z_ref, edge_ref,
    out_ref, push_ref, *, dims
):
    block, pack, own_y, rows, batch, parts = dims
    place = place_ref[0]
    for i in range(pack):
        near, far = near_ref[i], far_ref[i]
        diagonal = 1.0 + 2.0 * near
        at = [(place + (parts - b)) % parts for b in range(parts)]
        jumps = [rims_ref[at[b], 1, i] - rims_ref[at[b + 1], 0, i] for b in range(parts - 1)]
        ratio, value = [], []
        for j in range(parts - 1):
            pivot = diagonal if j == 0 else diagonal - far * ratio[-1]
            inverse = 1.0 / pivot
            ratio.append(far * inverse)
            value.append((jumps[j] if j == 0 else jumps[j] + far * value[-1]) * inverse)
        for j in range(parts - 3, -1, -1):
            value[j] = value[j] + ratio[j] * value[j + 1]
        left = jnp.zeros_like(near)
        right = jnp.zeros_like(near)
        for j in range(parts - 1):
            left = jnp.where(place == j + 1, value[j], left)
            right = jnp.where(place == j, -value[j], right)
        push_ref[0, i] = left
        push_ref[1, i] = right

    fill = edge_ref.shape[0] - 2 * pack

    def some(step, carry):
        solved = []
        for q in range(batch):
            k = step * batch + q
            pushes = [push_ref[e, i, pl.ds(k, 1), :] for e in range(2) for i in range(pack)]
            if fill:
                pushes.append(jnp.zeros((fill, rows), jnp.float32))
            push = jnp.concatenate(pushes, axis=0)
            spec = spec_ref[k] + dot(push.T, edge_ref[...])
            solved.append(spec / (plane_ref[...] + wave_z_ref[k, 0:1, :]))
        for q in range(batch):
            lines = product(halves(solved[q]), (cy_ref[0], cy_ref[1]), NN)
            stack = halves(rolled_stack(lines, pack, own_y))
            mixed = product((cx_ref[0], cx_ref[1]), stack, NN)
            out_ref[pl.ds(step * batch + q, rows, stride=block), :] = lane_group_select(
                mixed, pack, own_y
            )
        return carry

    lax.fori_loop(0, block // batch, some, 0)


def last_kernel(lines_ref, late_ref, cosine_ref, out_ref, *, dims):
    pack, own_y, tiles, batch = dims
    groups, packs, block, _ = lines_ref.shape

    def some(step, carry):
        for q in range(batch):
            xp = step * batch + q
            lines = jnp.concatenate(
                [ref[g, xp] for g in range(groups) for ref in (lines_ref, late_ref)], axis=0
            )
            values = product(halves(lines.T), (cosine_ref[0], cosine_ref[1]), NN)
            for j in range(pack):
                for h in range(tiles):
                    out_ref[h, xp * pack + j] = values[
                        j * own_y : (j + 1) * own_y, h * LANES : (h + 1) * LANES
                    ]
        return carry

    lax.fori_loop(0, packs // batch, some, 0)


def per_device(surface_ids, class_map, conductivity, normals, class_table):
    width_x, width_y, width_z = surface_ids.shape
    narrow, wide, outer = lax.axis_size("gz"), lax.axis_size("gy"), lax.axis_size("gx")
    length = width_z * narrow
    groups = outer * narrow
    own_x = width_x // narrow
    pack = LANES // width_y
    block = length // groups
    tiles = length // LANES
    part = block // 2
    rows = length // pack
    planes = own_x + 2 * HALO
    limit = 60 << 20

    class_value = jnp.zeros(class_map.shape, jnp.float32)
    for index in range(class_table.shape[0]):
        class_value = jnp.where(class_map == index, class_table[index], class_value)
    root = jnp.sqrt(class_value * conductivity)

    def split(values):
        values = values.reshape(narrow, own_x, width_y, width_z // LANES, LANES)
        return values.transpose(0, 3, 1, 2, 4)

    field = jnp.stack([split(surface_ids.astype(jnp.float32)), split(root)], axis=2)
    field = lax.all_to_all(field, "gz", split_axis=0, concat_axis=0, tiled=True)
    field = field.reshape(tiles, 2, own_x, width_y, LANES)

    axes = ("gx", "gy", "gz")

    def place(x, y):
        return (x // narrow * wide + y) * narrow + x % narrow

    def fetch(values, step_x, step_y):
        pairs = []
        for x in range(groups):
            for y in range(wide):
                if 0 <= x + step_x < groups and 0 <= y + step_y < wide:
                    pairs.append((place(x, y), place(x + step_x, y + step_y)))
        return lax.ppermute(values, axes, pairs)

    x_from = {1: slice(own_x - HALO, own_x), 0: slice(None), -1: slice(0, HALO)}
    y_from = {1: slice(width_y - HALO, width_y), 0: slice(None), -1: slice(0, HALO)}

    def beside(step_x, step_y):
        piece = field[:, :, x_from[step_x], y_from[step_y]]
        if step_y:
            piece = piece.reshape(tiles, 2, -1, LANES)
        return fetch(piece, step_x, step_y)

    pieces = [field] + [
        beside(*step)
        for step in ((1, 0), (-1, 0), (0, 1), (0, -1), (1, 1), (-1, 1), (1, -1), (-1, -1))
    ]
    extent = width_y + 2 * PAD + SUBLANES

    entries = normals.shape[1]
    table_blocks = -(-entries // LANES)
    table = jnp.pad(normals, ((0, 0), (0, table_blocks * LANES - entries)))
    table = jnp.broadcast_to(
        table.reshape(3, table_blocks, 1, LANES), (3, table_blocks, SUBLANES, LANES)
    )
    cosine = cosine_table(length)
    cells = np.arange(length) % LANES * tiles + np.arange(length) // LANES
    order = np.arange(length)[:, None] == cells[None, :]
    lines = pl.pallas_call(
        functools.partial(
            diffuse_kernel, dims=(tiles, planes, extent, own_x, width_y, pack, groups)
        ),
        out_shape=[jax.ShapeDtypeStruct((groups, own_x // pack, part, LANES), jnp.float32)] * 2,
        in_specs=[pl.BlockSpec(memory_space=pl.ANY)] * 3
        + [pl.BlockSpec(memory_space=pltpu.VMEM)] * 9,
        scratch_shapes=[
            pltpu.VMEM((tiles, 2, planes, extent, LANES), jnp.float32),
            pltpu.VMEM((3, tiles, planes, extent, LANES), jnp.float32),
            pltpu.VMEM((3, tiles, planes, extent, LANES), jnp.float32),
            pltpu.VMEM((tiles, planes, extent, LANES), jnp.float32),
            pltpu.VMEM((tiles, planes, extent, LANES), jnp.float32),
            pltpu.VMEM((3, tiles, width_y + 2 * SUBLANES, LANES), jnp.float32),
            pltpu.VMEM((3, tiles, width_y + 2 * SUBLANES, LANES), jnp.float32),
            pltpu.SemaphoreType.DMA((3,)),
        ],
        compiler_params=pltpu.CompilerParams(vmem_limit_bytes=limit),
        name="diffuse",
    )(*pieces, table, jnp.asarray(order.astype(jnp.bfloat16)), table_halves(cosine[:, cells]))

    def exchange(values):
        return lax.all_to_all(values, ("gx", "gz"), split_axis=0, concat_axis=0, tiled=True)

    lines = [exchange(half) for half in lines]

    spectra = eigen_values(length)
    screen = np.float32(4.0 / (length * length))
    local = exact_table(width_y)
    local_values = 2.0 - 2.0 * np.cos(np.pi * np.arange(width_y) / width_y)
    order_x = np.arange(rows) // (own_x // pack) * own_x + np.arange(rows) % (own_x // pack) * pack
    forward_x = np.zeros((pack, rows, pack, rows), np.float32)
    inverse_x = np.zeros((pack, rows, pack, rows), np.float32)
    for i in range(pack):
        for d in range(pack):
            other = (i - d) % pack
            forward_x[i, :, d, :] = cosine[i * rows : (i + 1) * rows][:, order_x + other]
            inverse_x[i, :, d, :] = cosine[other * rows : (other + 1) * rows][:, order_x + i].T
    forward_x = forward_x.reshape(length, length)
    inverse_x = inverse_x.reshape(length, length)
    eye = np.eye(pack)
    forward_y = np.kron(eye, -local.T).astype(np.float32)
    inverse_y = np.kron(eye, local).astype(np.float32)
    edge = np.concatenate([np.kron(eye, local[:, 0][None]), np.kron(eye, local[:, -1][None])])
    edge_rows = -(-2 * pack // SUBLANES) * SUBLANES
    edge = np.pad(edge, ((0, edge_rows - 2 * pack), (0, 0))).astype(np.float32)
    spectra_x = spectra.reshape(pack, rows)
    plane = (
        spectra_x.T[:, :, None] + local_values.astype(np.float32)[None, None, :] + screen
    ).reshape(rows, LANES)
    shift = (spectra[:, None].astype(np.float64) + spectra[None, :] + float(screen))[:, :, None]
    weights = 1.0 / (shift + local_values)
    near = (weights @ (local[:, 0] ** 2)).astype(np.float32)
    far = (weights @ (local[:, 0] * local[:, -1])).astype(np.float32)
    near = near.reshape(length, pack, rows).transpose(1, 0, 2)
    far = far.reshape(length, pack, rows).transpose(1, 0, 2)
    group = lax.axis_index("gx") * narrow + lax.axis_index("gz")
    near, far = (
        lax.dynamic_slice_in_dim(jnp.asarray(t), group * block, block, axis=1) for t in (near, far)
    )
    wave_z = lax.dynamic_slice_in_dim(jnp.asarray(spectra), group * block, block)
    wave_z = jnp.broadcast_to(wave_z[:, None, None], (block, SUBLANES, LANES))
    plane, edge = jnp.asarray(plane), jnp.asarray(edge)

    position = lax.axis_index("gy").reshape(1).astype(jnp.int32)
    tables = [table_halves(t) for t in (forward_x, forward_y, inverse_x, inverse_y)]

    def middle(lines, n):
        own_wave_z = wave_z[n * part : (n + 1) * part]
        spec, rim = pl.pallas_call(
            functools.partial(forward_kernel, dims=(part, pack, width_y, rows, 8)),
            out_shape=(
                jax.ShapeDtypeStruct((part, rows, LANES), jnp.float32),
                jax.ShapeDtypeStruct((2, pack, part, rows), jnp.float32),
            ),
            name="forward",
        )(lines.reshape(rows * part, LANES), tables[0], tables[1], plane, own_wave_z, edge)
        rims = jnp.stack(
            [rim]
            + [
                lax.ppermute(rim, "gy", [(i, (i + step) % wide) for i in range(wide)])
                for step in range(1, wide)
            ]
        )
        return spec, rims, own_wave_z

    def finish(spec, rims, own_wave_z, n):
        solved = pl.pallas_call(
            functools.partial(backward_kernel, dims=(part, pack, width_y, rows, 8, wide)),
            out_shape=jax.ShapeDtypeStruct((rows * part, LANES), jnp.float32),
            in_specs=[pl.BlockSpec(memory_space=pltpu.SMEM)]
            + [pl.BlockSpec(memory_space=pltpu.VMEM)] * 9,
            scratch_shapes=[pltpu.VMEM((2, pack, part, rows), jnp.float32)],
            name="backward",
        )(
            position, spec, rims, near[:, n * part : (n + 1) * part],
            far[:, n * part : (n + 1) * part], tables[2], tables[3], plane, own_wave_z, edge,
        )
        return exchange(solved.reshape(groups, own_x // pack, part, LANES))

    middles = [middle(half, n) for n, half in enumerate(lines)]
    lines = [finish(*values, n) for n, values in enumerate(middles)]
    distance = pl.pallas_call(
        functools.partial(last_kernel, dims=(pack, width_y, tiles, 2)),
        out_shape=jax.ShapeDtypeStruct((tiles, own_x, width_y, LANES), jnp.float32),
        name="last",
    )(*lines, table_halves(cosine))
    distance = distance.reshape(narrow, width_z // LANES, own_x, width_y, LANES)
    distance = lax.all_to_all(distance, "gz", split_axis=0, concat_axis=0, tiled=True)
    return distance.transpose(0, 2, 3, 1, 4).reshape(width_x, width_y, width_z)


def solution(mesh):
    in_specs = (P("gx", "gy", "gz"), P("gx", "gy", "gz"), P("gx", "gy", "gz"), P(), P())
    out_specs = P("gx", "gy", "gz")
    return jax.shard_map(
        per_device, mesh=mesh, in_specs=in_specs, out_specs=out_specs, check_vma=False
    )
```
